8 devices in a mesh: fsdp: 8 (over z, y, x, core).
Axes of the slice: x: 2, y: 2, z: 1, core: 2. Of those that a mesh axis runs over, the one named last changes fastest.
Arguments:
- hidden: bfloat16 [16, 1024, 2048], P('fsdp')
- norm_gain: bfloat16 [2048], P('fsdp')
- w_head: bfloat16 [32000, 2048], P('fsdp')
- labels: int32 [16, 1024], P('fsdp')
Outputs:
- output 1: float32 [], replicated
- output 2: bfloat16 [16, 1024, 2048], P('fsdp')
- output 3: float32 [32000, 2048], P('fsdp')
- output 4: float32 [2048], P('fsdp')
All inputs are finite; a program needn't handle non-finite values.
Results may differ from the reference program's by a relative error of at most 0.00857454.
Values are sent between devices in bfloat16 or wider.
A program may use at most 1 GiB of HBM per device.

```python
import jax
import jax.numpy as jnp
from jax import lax

HIDDEN = 2048
VOCAB_SIZE = 32000
BATCH_ALL = 16
SEQ_LEN = 1024
NUM_SHARDS = 8
ROW_BLOCK = 128
EPSILON = 1e-5
TOKENS = BATCH_ALL * SEQ_LEN
VOCAB_BLOCK = VOCAB_SIZE // NUM_SHARDS
ROWS_DEV = BATCH_ALL // NUM_SHARDS


def draw_labels(label_key):
    k_shift, k_row, k_perm, k_tok = jax.random.split(label_key, 4)
    tok_index = jnp.arange(TOKENS, dtype=jnp.int32).reshape(BATCH_ALL, SEQ_LEN)
    tok_shift = jax.random.randint(k_shift, (), 0, NUM_SHARDS)
    block_id = (tok_index + tok_shift) % NUM_SHARDS
    within = jax.random.randint(k_row, (BATCH_ALL, SEQ_LEN), 0, VOCAB_BLOCK)
    target = block_id * VOCAB_BLOCK + within
    shard_rank = jax.random.permutation(k_perm, NUM_SHARDS)
    percent = shard_rank * 60 // (NUM_SHARDS - 1)
    row_percent = jnp.repeat(percent, ROWS_DEV)[:, None]
    draw_pct = jax.random.randint(k_tok, (BATCH_ALL, SEQ_LEN), 0, 100)
    return jnp.where(draw_pct < row_percent, -100, target).astype(jnp.int32)


def setup_inputs(seed: int = 0) -> dict:
    root_key = jax.random.key(seed)
    k_h, k_g, k_w, k_lab = jax.random.split(root_key, 4)
    hidden = jax.random.normal(k_h, (BATCH_ALL, SEQ_LEN, HIDDEN), jnp.float32)
    norm_gain = 1.0 + 0.5 * jax.random.normal(k_g, (HIDDEN,), jnp.float32)
    w_head = (2.0 / HIDDEN ** 0.5) * jax.random.normal(k_w, (VOCAB_SIZE, HIDDEN), jnp.float32)
    return {'hidden': hidden.astype(jnp.bfloat16), 'norm_gain': norm_gain.astype(jnp.bfloat16), 'w_head': w_head.astype(jnp.bfloat16), 'labels': draw_labels(k_lab)}


def reference(hidden, norm_gain, w_head, labels):
    is_valid = labels >= 0
    tok_count = jnp.sum(is_valid.astype(jnp.float32))
    gain_f32 = norm_gain.astype(jnp.float32)
    vocab_ids = jnp.arange(VOCAB_SIZE, dtype=jnp.int32)
    h_blocks = hidden.reshape(TOKENS // ROW_BLOCK, ROW_BLOCK, HIDDEN)
    lab_blocks = labels.reshape(TOKENS // ROW_BLOCK, ROW_BLOCK)

    def block_step(acc_state, block_in):
        loss_sum, dw_acc, dg_acc = acc_state
        h_blk, lab_blk = block_in
        h_f32 = h_blk.astype(jnp.float32)
        inv_rms = lax.rsqrt(jnp.mean(h_f32 * h_f32, axis=-1, keepdims=True) + EPSILON)
        normed = (h_f32 * inv_rms).astype(jnp.bfloat16)
        x_in = (normed.astype(jnp.float32) * gain_f32).astype(jnp.bfloat16)
        logits = jnp.dot(x_in, w_head.T, preferred_element_type=jnp.float32)
        row_max = jnp.max(logits, axis=-1, keepdims=True)
        shifted = jnp.exp(logits - row_max)
        sum_exp = jnp.sum(shifted, axis=-1, keepdims=True)
        log_norm = row_max[:, 0] + jnp.log(sum_exp[:, 0])
        onehot = vocab_ids[None, :] == lab_blk[:, None]
        picked = jnp.sum(jnp.where(onehot, logits, 0.0), axis=-1)
        blk_valid = lab_blk >= 0
        loss_sum = loss_sum + jnp.sum(jnp.where(blk_valid, log_norm - picked, 0.0))
        dlogits = jnp.where(blk_valid[:, None], shifted / sum_exp - onehot.astype(jnp.float32), 0.0) / tok_count
        dlog_bf = dlogits.astype(jnp.bfloat16)
        grad_x = jnp.dot(dlog_bf, w_head, preferred_element_type=jnp.float32).astype(jnp.bfloat16)
        dw_acc = dw_acc + jnp.dot(dlog_bf.T, x_in, preferred_element_type=jnp.float32)
        gx_f32 = grad_x.astype(jnp.float32)
        dg_acc = dg_acc + jnp.sum(gx_f32 * normed.astype(jnp.float32), axis=0)
        grad_n = gx_f32 * gain_f32
        dot_proj = jnp.mean(grad_n * h_f32, axis=-1, keepdims=True)
        grad_h = (inv_rms * grad_n - h_f32 * inv_rms ** 3 * dot_proj).astype(jnp.bfloat16)
        return (loss_sum, dw_acc, dg_acc), grad_h

    init_state = (jnp.zeros((), jnp.float32), jnp.zeros((VOCAB_SIZE, HIDDEN), jnp.float32), jnp.zeros((HIDDEN,), jnp.float32))
    final_state, grad_blocks = lax.scan(block_step, init_state, (h_blocks, lab_blocks))
    loss_sum, grad_w, grad_g = final_state
    return (loss_sum / tok_count, grad_blocks.reshape(BATCH_ALL, SEQ_LEN, HIDDEN), grad_w, grad_g)
```

```python
import functools

import jax
import jax.numpy as jnp
from jax import lax
from jax.experimental import pallas as pl
from jax.experimental.pallas import tpu as pltpu
from jax.sharding import PartitionSpec as P


EPSILON = 1e-5

AX = "fsdp"
NDEV = 8
D = 2048
VD = 4000
VC = 8000
CH = 512
HF = CH // 2
NCH = 4
VB1 = 800
VB2 = 1000
SUB = 80
F32 = jnp.float32
BF16 = jnp.bfloat16
VMEM_LIMIT = 63 * 2 ** 20
NB1 = VC // VB1
NB2 = VC // VB2


def logits_kernel(moves, aliased, ndep, core_ref, w_ref, *refs):
    nx = len(moves)
    xs, refs = refs[:nx], refs[nx + ndep + (1 if aliased else 0):]
    l_ref, lse_ref, x_all, x_ref, m_ref, s_ref, sems = refs
    v = pl.program_id(0)
    flat = [(x, mv) for x, mvs in zip(xs, moves) for mv in mvs]
    loads = [pltpu.make_async_copy(x.at[pl.ds(a, n), :], x_ref.at[pl.ds(b, n), :], sems.at[0, i]) for i, (x, (a, b, _, n)) in enumerate(flat)]
    saves = [pltpu.make_async_copy(x_ref.at[pl.ds(b, n), :], x_all.at[pl.ds(g, n), :], sems.at[1, i]) for i, (_, (_, b, g, n)) in enumerate(flat)]

    @pl.when(v == 0)
    def _():
        for cp in loads:
            cp.start()
        m_ref[...] = jnp.full_like(m_ref, -jnp.inf)
        s_ref[...] = jnp.zeros_like(s_ref)
        for cp in loads:
            cp.wait()
        for cp in saves:
            cp.start()

    l = lax.dot_general(w_ref[...], x_ref[...], (((1,), (1,)), ((), ())), preferred_element_type=F32)
    l_ref[...] = l
    m, s = m_ref[...], s_ref[...]
    for q in range(VB1 // SUB):
        blk = l[q * SUB:(q + 1) * SUB]
        m_new = jnp.maximum(m, jnp.max(blk, axis=0, keepdims=True))
        s = s * jnp.exp(m - m_new) + jnp.sum(jnp.exp(blk - m_new), axis=0, keepdims=True)
        m = m_new
    m_ref[...] = m
    s_ref[...] = s

    @pl.when(v == pl.num_programs(0) - 1)
    def _():
        lse_ref[...] = m_ref[...] + jnp.log(s_ref[...])
        for cp in saves:
            cp.wait()


def local_logits(core, w, xs, moves, x_all, deps):
    t = NCH * CH
    half = NB1 // 2
    nmv = sum(len(m) for m in moves)
    anywhere = pl.BlockSpec(memory_space=pl.ANY)
    args = [core, w, *xs, *deps]
    aliases = {}
    if x_all is not None:
        aliases = {len(args): 2}
        args.append(x_all)
    return pl.pallas_call(
        functools.partial(logits_kernel, moves, x_all is not None, len(deps)),
        grid_spec=pltpu.PrefetchScalarGridSpec(
            num_scalar_prefetch=1,
            grid=(NB1,),
            in_specs=[pl.BlockSpec((VB1, D), lambda v, c: (lax.rem(v + half * c[0], NB1), 0))] + [anywhere] * (len(args) - 2),
            out_specs=[pl.BlockSpec((VB1, t), lambda v, c: (v, 0)), pl.BlockSpec((1, t), lambda v, c: (0, 0)), anywhere],
            scratch_shapes=[pltpu.VMEM((t, D), BF16), pltpu.VMEM((1, t), F32), pltpu.VMEM((1, t), F32), pltpu.SemaphoreType.DMA((2, nmv))],
        ),
        out_shape=(jax.ShapeDtypeStruct((VC, t), F32), jax.ShapeDtypeStruct((1, t), F32), jax.ShapeDtypeStruct((NCH * 4 * CH, D), BF16)),
        input_output_aliases=aliases,
        compiler_params=pltpu.CompilerParams(vmem_limit_bytes=VMEM_LIMIT, dimension_semantics=("arbitrary",)),
        cost_estimate=pl.CostEstimate(flops=2 * VC * t * D, bytes_accessed=VC * t * 4 + VC * D * 2, transcendentals=VC * t),
    )(*args)


def grad_kernel(widths, outs, nskip, core_ref, w_ref, lab_ref, lse_ref, sc_ref, *refs):
    nl = len(widths)
    ls, refs = refs[:nl], refs[nl:]
    refs = refs[nskip:]
    dz_ref, pk_ref, dxs = refs[0], refs[1], refs[2:]
    v = pl.program_id(0)

    @pl.when(v == 0)
    def _():
        pk_ref[...] = jnp.zeros_like(pk_ref)
        for dx_ref in dxs:
            dx_ref[...] = jnp.zeros_like(dx_ref)

    col = 0
    for l_ref, width in zip(ls, widths):
        cols = pl.ds(col, width)
        lab = lab_ref[:, cols] - v * VB2
        lse, sc = lse_ref[:, cols], sc_ref[:, cols]
        pk = pk_ref[:, cols]
        for q in range(0, VB2, SUB):
            size = min(SUB, VB2 - q)
            rows = pl.ds(q, size)
            l = l_ref[rows, :]
            hit = lax.broadcasted_iota(jnp.int32, (size, width), 0) == lab - q
            e = jnp.exp(l - lse)
            pk = pk + jnp.sum(jnp.where(hit, l, 0.0), axis=0, keepdims=True)
            dz_ref[rows, cols] = (jnp.where(hit, e - 1.0, e) * sc).astype(BF16)
        pk_ref[:, cols] = pk
        col += width
    dx = lax.dot_general(dz_ref[...], w_ref[...], (((0,), (0,)), ((), ())), preferred_element_type=F32)
    for dx_ref, pieces in zip(dxs, outs):
        for src, dst, n in pieces:
            dx_ref[pl.ds(dst, n), :] += dx[src:src + n]


def local_grads(core, w, lab, lse, sc, ls, dz_all, slot, outs, deps):
    t = sum(width for _, width, _ in ls)
    half = NB2 // 2
    row = pl.BlockSpec((1, t), lambda v, c: (0, 0))
    in_specs = [pl.BlockSpec((VB2, D), lambda v, c: (lax.rem(v + half * c[0], NB2), 0)), row, row, row]
    in_specs += [pl.BlockSpec((VB2, width), lambda v, c, b=block: (v, b)) for _, width, block in ls]
    args = [core, w, lab, lse, sc] + [a for a, _, _ in ls] + list(deps)
    aliases = {}
    if dz_all is not None:
        aliases = {len(args): 0}
        args.append(dz_all)
    extra = len(args) - 1 - len(in_specs)
    in_specs += [pl.BlockSpec(memory_space=pl.ANY)] * extra
    heights = [sum(n for _, _, n in pieces) for pieces in outs]
    return pl.pallas_call(
        functools.partial(grad_kernel, tuple(width for _, width, _ in ls), outs, extra),
        grid_spec=pltpu.PrefetchScalarGridSpec(
            num_scalar_prefetch=1,
            grid=(NB2,),
            in_specs=in_specs,
            out_specs=[pl.BlockSpec((VB2, t), lambda v, c: (v, slot)), row] + [pl.BlockSpec((n, D), lambda v, c: (0, 0)) for n in heights],
        ),
        out_shape=[jax.ShapeDtypeStruct((VC, NCH * 4 * CH), BF16), jax.ShapeDtypeStruct((1, t), F32)]
        + [jax.ShapeDtypeStruct((n, D), F32) for n in heights],
        input_output_aliases=aliases,
        compiler_params=pltpu.CompilerParams(vmem_limit_bytes=VMEM_LIMIT, dimension_semantics=("arbitrary",)),
        cost_estimate=pl.CostEstimate(flops=2 * VC * t * D, bytes_accessed=VC * t * 6 + VC * D * 2, transcendentals=VC * t),
    )(*args)


def hop(a, bit):
    return lax.ppermute(a, AX, [(d, d ^ bit) for d in range(NDEV)])


OWN, XN, YN, DG = 0, 1, 2, 3
ORDER = [(XN, 0), (YN, 1), (DG, 0), (DG, 1), (YN, 0), (XN, 1), (OWN, 0), (OWN, 1)]
POS = {rs: i for i, rs in enumerate(ORDER)}


def in_order(a):
    h = a.reshape(4, 2, HF)
    return jnp.concatenate([h[r, s] for r, s in ORDER])[None]


def by_owner(cols):
    h = cols.reshape(8, HF)
    return jnp.stack([h[POS[r, s]] for r in range(4) for s in range(2)]).reshape(4, CH)


def after(a, *deps):
    return lax.optimization_barrier((a, *deps))[0]


def solution(mesh):
    def local_step(hidden, norm_gain, w_head, labels):
        nb, seq_len, _ = hidden.shape
        me = lax.axis_index(AX)
        core = lax.rem(me, 2)
        chip = me // 2

        w2 = lax.all_gather(w_head, AX, axis=0, tiled=True, axis_index_groups=[[2 * k, 2 * k + 1] for k in range(4)])
        small = jnp.concatenate([labels.reshape(-1).astype(F32), norm_gain.astype(F32)])
        small = lax.all_gather(small, AX, axis=0)
        lab_all = small[:, :nb * seq_len].astype(jnp.int32)
        gain = small[:, nb * seq_len:].reshape(1, D)
        count = jnp.sum((lab_all >= 0).astype(F32))

        h_c = hidden.reshape(NCH, CH, D)
        x_own = []
        for c in range(NCH):
            h = h_c[c].astype(F32)
            r = lax.rsqrt(jnp.mean(h * h, axis=-1, keepdims=True) + EPSILON)
            n = (h * r).astype(BF16)
            x_own.append((n.astype(F32) * gain).astype(BF16))

        core_arr = core[None].astype(jnp.int32)

        def whole(c, r, block):
            return [(0, block * CH, c * 4 * CH + POS[r, 0] * HF, CH)]

        def split(c, r, block):
            first = [(XN, 0), (YN, 1)]
            out = []
            for s in range(2):
                lead = (r, s) in first
                col = (0 if lead else CH) + ([XN, YN].index(r) if lead else [YN, XN].index(r)) * HF
                out.append((s * HF, block * CH + col, c * 4 * CH + POS[r, s] * HF, HF))
            return out

        x_x = [hop(x_own[c], 2) for c in range(3)]
        x_y = [hop(x_own[c], 4) for c in range(3)]
        l_own, lse_own, x_all = local_logits(core_arr, w2, x_own, [whole(c, OWN, c) for c in range(NCH)], None, [])
        late = after(x_own[3], lse_own)
        x_x.append(hop(late, 2))
        x_y.append(hop(late, 4))
        x_d = [hop(after(x_y[c], lse_own), 2) if c % 2 == 0 else hop(after(x_x[c], lse_own), 4) for c in range(2)]
        l_1, lse_1, x_all = local_logits(
            core_arr, w2, [x_x[0], x_y[0], x_x[1], x_y[1]],
            [split(0, XN, 0), split(0, YN, 0), split(1, XN, 2), split(1, YN, 2)], x_all, [])
        x_d.append(hop(after(x_y[2], lse_1), 2))
        l_2, lse_2, x_all = local_logits(
            core_arr, w2, [x_d[0], x_d[1], x_x[2], x_y[2]],
            [whole(0, DG, 0), whole(1, DG, 1), split(2, XN, 2), split(2, YN, 2)], x_all, [])
        x_d.append(hop(after(x_x[3], lse_2), 4))

        def full_lse(blocks):
            mine = jnp.stack([by_owner(jnp.concatenate(b)) for b in blocks], axis=1)
            parts = [mine] + [hop(mine, q << 1)[jnp.array([r ^ q for r in range(4)])] for q in (1, 2, 3)]
            stack = jnp.stack(parts)
            top = jnp.max(stack, axis=0)
            full = top + jnp.log(jnp.sum(jnp.exp(stack - top), axis=0))
            return [in_order(full[:, i]) for i in range(len(blocks))]

        def blk(a, i):
            return a[0, i * CH:(i + 1) * CH]

        owners = jnp.stack([me ^ (r << 1) for r in range(4)])
        lab_grp = lab_all[owners].reshape(4, NCH, CH)
        local = lab_grp - chip * VC
        here = (local >= 0) & (local < VC)
        row = jnp.where(here, lax.rem(local + VC - core * VD, VC), -1)
        scale = jnp.where(lab_grp >= 0, 1.0 / count, 0.0)
        lab_c = [in_order(row[:, c]) for c in range(NCH)]
        sc_c = [in_order(scale[:, c]) for c in range(NCH)]

        lse_c = full_lse([
            [blk(lse_1, 0), blk(lse_2, 0), blk(lse_1, 1), blk(lse_own, 0)],
            [blk(lse_1, 2), blk(lse_2, 1), blk(lse_1, 3), blk(lse_own, 1)]])
        t = 2 * CH
        send_outs = (((0, 0, HF), (CH, HF, HF)), ((HF, 0, HF), (CH + HF, HF, HF)))
        keep_outs = (((0, 0, HF),), ((HF, 0, HF),), ((CH, 0, CH),))
        l_xy = [(l_1, 0), (l_1, 2), (l_2, 2), None]
        l_dg = [(l_2, 0), (l_2, 1), None, None]
        dz_all, loss_sum = None, 0.0
        dx_own, arrived, pending = [], [], []

        def forward(c):
            (in_a, in_b), (k_y, k_x, k_own) = arrived[c]
            add_a, add_b = k_y + in_a[HF:], k_x + in_b[HF:]
            pending.append((hop(add_a, 4), hop(add_b, 2)))
            return [add_a, add_b]

        for c in range(NCH):
            deps_out, deps_keep = [], []
            if c == 1:
                deps_out = [lse_3] + forward(0)
            if c == 2:
                deps_out = list(pending[0])
            if c >= 2:
                deps_keep = forward(c - 1)
            (a_xy, b_xy), (a_dg, b_dg) = l_xy[c], l_dg[c]
            dz_all, pk1, send_a, send_b = local_grads(
                core_arr, w2, lab_c[c][:, :t], lse_c[c][:, :t], sc_c[c][:, :t], [(a_xy, CH, b_xy), (a_dg, CH, b_dg)], dz_all, 2 * c,
                send_outs, deps_out)
            incoming = (hop(send_a, 2), hop(send_b, 4))
            dz_all, pk2, k_y, k_x, k_own = local_grads(
                core_arr, w2, lab_c[c][:, t:], lse_c[c][:, t:], sc_c[c][:, t:], [(a_xy, CH, b_xy + 1), (l_own, CH, c)], dz_all, 2 * c + 1,
                keep_outs, deps_keep)
            arrived.append((incoming, (k_y, k_x, k_own)))
            pk = jnp.concatenate([pk1, pk2], axis=1)
            loss_sum = loss_sum + jnp.sum(jnp.where(lab_c[c] >= 0, lse_c[c] - pk, 0.0))
            if c == 0:
                l_3, lse_3, x_all = local_logits(
                    core_arr, w2, [x_d[2], x_d[3], x_x[3], x_y[3]],
                    [whole(2, DG, 0), whole(3, DG, 1), split(3, XN, 2), split(3, YN, 2)], x_all, [pk2])
                l_dg[2:] = [(l_3, 0), (l_3, 1)]
                l_xy[3] = (l_3, 2)
                lse_c += full_lse([
                    [blk(lse_2, 2), blk(lse_3, 0), blk(lse_2, 3), blk(lse_own, 2)],
                    [blk(lse_3, 2), blk(lse_3, 1), blk(lse_3, 3), blk(lse_own, 3)]])

        def dw_part(rows, cols):
            return jnp.einsum("vt,td->vd", dz_all[rows, cols], x_all[cols], preferred_element_type=F32)

        every, head, rest = slice(None), slice(0, 2 * NCH * CH), slice(2 * NCH * CH, None)
        dz_all, *pending[1] = lax.optimization_barrier((dz_all, *pending[1]))
        dw_other = dw_part(slice(VD, None), every)
        arrived[3] = after(arrived[3], dw_other[:8, :128])
        forward(NCH - 1)
        dw_other = hop(dw_other, 1)
        x_all, *pending[2] = lax.optimization_barrier((x_all, *pending[2]))
        dw_mine = dw_part(slice(0, VD), head)
        pending[3] = after(pending[3], dw_mine[:8, :128])

        for c in range(NCH):
            (in_a, in_b), (_, _, k_own) = arrived[c]
            fin_a, fin_b = pending[c]
            dx_own.append(jnp.concatenate([k_own[:HF] + in_a[:HF] + fin_a, k_own[HF:] + in_b[:HF] + fin_b]))

        dg, dh = 0.0, []
        for c in range(NCH):
            gx = dx_own[c].astype(BF16).astype(F32)
            h = h_c[c].astype(F32)
            r = lax.rsqrt(jnp.mean(h * h, axis=-1, keepdims=True) + EPSILON)
            n = (h * r).astype(BF16).astype(F32)
            dg = dg + jnp.sum(gx * n, axis=0)
            gn = gx * gain
            proj = jnp.mean(gn * h, axis=-1, keepdims=True)
            dh.append((r * gn - h * r ** 3 * proj).astype(BF16))
        dz_all, dg = lax.optimization_barrier((dz_all, dg))
        grad_w = dw_part(slice(0, VD), rest) + (dw_mine + dw_other)
        tail = lax.psum(jnp.concatenate([dg, jnp.full((128,), loss_sum, F32)]), AX)
        grad_g = lax.dynamic_slice(tail, (me * (D // NDEV),), (D // NDEV,))
        loss_value = tail[D] / count
        return loss_value, jnp.concatenate(dh).reshape(nb, seq_len, D), grad_w, grad_g

    return jax.shard_map(local_step, mesh=mesh, in_specs=(P(AX, None, None), P(AX), P(AX, None), P(AX, None)), out_specs=(P(), P(AX, None, None), P(AX, None), P(AX)), check_vma=False)
```

```python
import functools

import jax
import jax.numpy as jnp
from jax import lax
from jax.experimental import pallas as pl
from jax.experimental.pallas import tpu as pltpu
from jax.sharding import PartitionSpec as P


EPSILON = 1e-5

AX = "fsdp"
NDEV = 8
D = 2048
VD = 4000
VC = 8000
CH = 512
HF = CH // 2
NCH = 4
VB1 = 800
VB2 = 1000
SUB = 80
F32 = jnp.float32
BF16 = jnp.bfloat16
VMEM_LIMIT = 63 * 2 ** 20
NB1 = VC // VB1
NB2 = VC // VB2


def logits_kernel(moves, aliased, ndep, core_ref, w_ref, *refs):
    nx = len(moves)
    xs, refs = refs[:nx], refs[nx + ndep + (1 if aliased else 0):]
    l_ref, lse_ref, x_all, x_ref, m_ref, s_ref, sems = refs
    v = pl.program_id(0)
    flat = [(x, mv) for x, mvs in zip(xs, moves) for mv in mvs]
    loads = [pltpu.make_async_copy(x.at[pl.ds(a, n), :], x_ref.at[pl.ds(b, n), :], sems.at[0, i]) for i, (x, (a, b, _, n)) in enumerate(flat)]
    saves = [pltpu.make_async_copy(x_ref.at[pl.ds(b, n), :], x_all.at[pl.ds(g, n), :], sems.at[1, i]) for i, (_, (_, b, g, n)) in enumerate(flat)]

    @pl.when(v == 0)
    def _():
        for cp in loads:
            cp.start()
        m_ref[...] = jnp.full_like(m_ref, -jnp.inf)
        s_ref[...] = jnp.zeros_like(s_ref)
        for cp in loads:
            cp.wait()
        for cp in saves:
            cp.start()

    l = lax.dot_general(w_ref[...], x_ref[...], (((1,), (1,)), ((), ())), preferred_element_type=F32)
    l_ref[...] = l
    m, s = m_ref[...], s_ref[...]
    for q in range(VB1 // SUB):
        blk = l[q * SUB:(q + 1) * SUB]
        m_new = jnp.maximum(m, jnp.max(blk, axis=0, keepdims=True))
        s = s * jnp.exp(m - m_new) + jnp.sum(jnp.exp(blk - m_new), axis=0, keepdims=True)
        m = m_new
    m_ref[...] = m
    s_ref[...] = s

    @pl.when(v == pl.num_programs(0) - 1)
    def _():
        lse_ref[...] = m_ref[...] + jnp.log(s_ref[...])
        for cp in saves:
            cp.wait()


def local_logits(core, w, xs, moves, x_all, deps):
    t = NCH * CH
    half = NB1 // 2
    nmv = sum(len(m) for m in moves)
    anywhere = pl.BlockSpec(memory_space=pl.ANY)
    args = [core, w, *xs, *deps]
    aliases = {}
    if x_all is not None:
        aliases = {len(args): 2}
        args.append(x_all)
    return pl.pallas_call(
        functools.partial(logits_kernel, moves, x_all is not None, len(deps)),
        grid_spec=pltpu.PrefetchScalarGridSpec(
            num_scalar_prefetch=1,
            grid=(NB1,),
            in_specs=[pl.BlockSpec((VB1, D), lambda v, c: (lax.rem(v + half * c[0], NB1), 0))] + [anywhere] * (len(args) - 2),
            out_specs=[pl.BlockSpec((VB1, t), lambda v, c: (v, 0)), pl.BlockSpec((1, t), lambda v, c: (0, 0)), anywhere],
            scratch_shapes=[pltpu.VMEM((t, D), BF16), pltpu.VMEM((1, t), F32), pltpu.VMEM((1, t), F32), pltpu.SemaphoreType.DMA((2, nmv))],
        ),
        out_shape=(jax.ShapeDtypeStruct((VC, t), F32), jax.ShapeDtypeStruct((1, t), F32), jax.ShapeDtypeStruct((NCH * 4 * CH, D), BF16)),
        input_output_aliases=aliases,
        compiler_params=pltpu.CompilerParams(vmem_limit_bytes=VMEM_LIMIT, dimension_semantics=("arbitrary",)),
        cost_estimate=pl.CostEstimate(flops=2 * VC * t * D, bytes_accessed=VC * t * 4 + VC * D * 2, transcendentals=VC * t),
    )(*args)


def grad_kernel(widths, outs, nskip, core_ref, w_ref, lab_ref, lse_ref, sc_ref, *refs):
    nl = len(widths)
    ls, refs = refs[:nl], refs[nl:]
    refs = refs[nskip:]
    dz_ref, pk_ref, dxs = refs[0], refs[1], refs[2:]
    v = pl.program_id(0)

    @pl.when(v == 0)
    def _():
        pk_ref[...] = jnp.zeros_like(pk_ref)
        for dx_ref in dxs:
            dx_ref[...] = jnp.zeros_like(dx_ref)

    col = 0
    for l_ref, width in zip(ls, widths):
        cols = pl.ds(col, width)
        lab = lab_ref[:, cols] - v * VB2
        lse, sc = lse_ref[:, cols], sc_ref[:, cols]
        pk = pk_ref[:, cols]
        for q in range(0, VB2, SUB):
            size = min(SUB, VB2 - q)
            rows = pl.ds(q, size)
            l = l_ref[rows, :]
            hit = lax.broadcasted_iota(jnp.int32, (size, width), 0) == lab - q
            e = jnp.exp(l - lse)
            pk = pk + jnp.sum(jnp.where(hit, l, 0.0), axis=0, keepdims=True)
            dz_ref[rows, cols] = (jnp.where(hit, e - 1.0, e) * sc).astype(BF16)
        pk_ref[:, cols] = pk
        col += width
    dx = lax.dot_general(dz_ref[...], w_ref[...], (((0,), (0,)), ((), ())), preferred_element_type=F32)
    for dx_ref, pieces in zip(dxs, outs):
        for src, dst, n in pieces:
            dx_ref[pl.ds(dst, n), :] += dx[src:src + n]


def local_grads(core, w, lab, lse, sc, ls, dz_all, slot, outs, deps):
    t = sum(width for _, width, _ in ls)
    half = NB2 // 2
    row = pl.BlockSpec((1, t), lambda v, c: (0, 0))
    in_specs = [pl.BlockSpec((VB2, D), lambda v, c: (lax.rem(v + half * c[0], NB2), 0)), row, row, row]
    in_specs += [pl.BlockSpec((VB2, width), lambda v, c, b=block: (v, b)) for _, width, block in ls]
    args = [core, w, lab, lse, sc] + [a for a, _, _ in ls] + list(deps)
    aliases = {}
    if dz_all is not None:
        aliases = {len(args): 0}
        args.append(dz_all)
    extra = len(args) - 1 - len(in_specs)
    in_specs += [pl.BlockSpec(memory_space=pl.ANY)] * extra
    heights = [sum(n for _, _, n in pieces) for pieces in outs]
    return pl.pallas_call(
        functools.partial(grad_kernel, tuple(width for _, width, _ in ls), outs, extra),
        grid_spec=pltpu.PrefetchScalarGridSpec(
            num_scalar_prefetch=1,
            grid=(NB2,),
            in_specs=in_specs,
            out_specs=[pl.BlockSpec((VB2, t), lambda v, c: (v, slot)), row] + [pl.BlockSpec((n, D), lambda v, c: (0, 0)) for n in heights],
        ),
        out_shape=[jax.ShapeDtypeStruct((VC, NCH * 4 * CH), BF16), jax.ShapeDtypeStruct((1, t), F32)]
        + [jax.ShapeDtypeStruct((n, D), F32) for n in heights],
        input_output_aliases=aliases,
        compiler_params=pltpu.CompilerParams(vmem_limit_bytes=VMEM_LIMIT, dimension_semantics=("arbitrary",)),
        cost_estimate=pl.CostEstimate(flops=2 * VC * t * D, bytes_accessed=VC * t * 6 + VC * D * 2, transcendentals=VC * t),
    )(*args)


def hop(a, bit):
    return lax.ppermute(a, AX, [(d, d ^ bit) for d in range(NDEV)])


OWN, XN, YN, DG = 0, 1, 2, 3
ORDER = [(XN, 0), (YN, 1), (DG, 0), (DG, 1), (YN, 0), (XN, 1), (OWN, 0), (OWN, 1)]
POS = {rs: i for i, rs in enumerate(ORDER)}


def in_order(a):
    h = a.reshape(4, 2, HF)
    return jnp.concatenate([h[r, s] for r, s in ORDER])[None]


def by_owner(cols):
    h = cols.reshape(8, HF)
    return jnp.stack([h[POS[r, s]] for r in range(4) for s in range(2)]).reshape(4, CH)


def after(a, *deps):
    return lax.optimization_barrier((a, *deps))[0]


def solution(mesh):
    def local_step(hidden, norm_gain, w_head, labels):
        nb, seq_len, _ = hidden.shape
        me = lax.axis_index(AX)
        core = lax.rem(me, 2)
        chip = me // 2

        w2 = lax.all_gather(w_head, AX, axis=0, tiled=True, axis_index_groups=[[2 * k, 2 * k + 1] for k in range(4)])
        small = jnp.concatenate([labels.reshape(-1).astype(F32), norm_gain.astype(F32)])
        small = lax.all_gather(small, AX, axis=0)
        lab_all = small[:, :nb * seq_len].astype(jnp.int32)
        gain = small[:, nb * seq_len:].reshape(1, D)
        count = jnp.sum((lab_all >= 0).astype(F32))

        h_c = hidden.reshape(NCH, CH, D)
        x_own = []
        for c in range(NCH):
            h = h_c[c].astype(F32)
            r = lax.rsqrt(jnp.mean(h * h, axis=-1, keepdims=True) + EPSILON)
            n = (h * r).astype(BF16)
            x_own.append((n.astype(F32) * gain).astype(BF16))

        core_arr = core[None].astype(jnp.int32)

        def whole(c, r, block):
            return [(0, block * CH, c * 4 * CH + POS[r, 0] * HF, CH)]

        def split(c, r, block):
            first = [(XN, 0), (YN, 1)]
            out = []
            for s in range(2):
                lead = (r, s) in first
                col = (0 if lead else CH) + ([XN, YN].index(r) if lead else [YN, XN].index(r)) * HF
                out.append((s * HF, block * CH + col, c * 4 * CH + POS[r, s] * HF, HF))
            return out

        x_x = [hop(x_own[c], 2) for c in range(2)]
        x_y = [hop(x_own[c], 4) for c in range(2)]
        l_own, lse_own, x_all = local_logits(core_arr, w2, x_own, [whole(c, OWN, c) for c in range(NCH)], None, [])
        x_d = [hop(after(x_y[0], lse_own), 2), hop(after(x_x[1], lse_own), 4)]
        late = after(x_own[2], lse_own)
        x_x.append(hop(late, 2))
        x_y.append(hop(late, 4))
        l_1, lse_1, x_all = local_logits(
            core_arr, w2, [x_x[0], x_y[0], x_x[1], x_y[1]],
            [split(0, XN, 0), split(0, YN, 0), split(1, XN, 2), split(1, YN, 2)], x_all, [])
        late = after(x_own[3], lse_1)
        x_x.append(hop(late, 2))
        x_y.append(hop(late, 4))
        x_d.append(hop(after(x_y[2], lse_1), 2))
        l_2, lse_2, x_all = local_logits(
            core_arr, w2, [x_d[0], x_d[1], x_x[2], x_y[2]],
            [whole(0, DG, 0), whole(1, DG, 1), split(2, XN, 2), split(2, YN, 2)], x_all, [])
        x_d.append(hop(after(x_x[3], lse_2), 4))

        def full_lse(blocks):
            mine = jnp.stack([by_owner(jnp.concatenate(b)) for b in blocks], axis=1)
            parts = [mine] + [hop(mine, q << 1)[jnp.array([r ^ q for r in range(4)])] for q in (1, 2, 3)]
            stack = jnp.stack(parts)
            top = jnp.max(stack, axis=0)
            full = top + jnp.log(jnp.sum(jnp.exp(stack - top), axis=0))
            return [in_order(full[:, i]) for i in range(len(blocks))]

        def blk(a, i):
            return a[0, i * CH:(i + 1) * CH]

        owners = jnp.stack([me ^ (r << 1) for r in range(4)])
        lab_grp = lab_all[owners].reshape(4, NCH, CH)
        local = lab_grp - chip * VC
        here = (local >= 0) & (local < VC)
        row = jnp.where(here, lax.rem(local + VC - core * VD, VC), -1)
        scale = jnp.where(lab_grp >= 0, 1.0 / count, 0.0)
        lab_c = [in_order(row[:, c]) for c in range(NCH)]
        sc_c = [in_order(scale[:, c]) for c in range(NCH)]

        lse_c = full_lse([
            [blk(lse_1, 0), blk(lse_2, 0), blk(lse_1, 1), blk(lse_own, 0)],
            [blk(lse_1, 2), blk(lse_2, 1), blk(lse_1, 3), blk(lse_own, 1)]])
        t = 2 * CH
        send_outs = (((0, 0, HF), (CH, HF, HF)), ((HF, 0, HF), (CH + HF, HF, HF)))
        keep_outs = (((0, 0, HF),), ((HF, 0, HF),), ((CH, 0, CH),))
        l_xy = [(l_1, 0), (l_1, 2), (l_2, 2), None]
        l_dg = [(l_2, 0), (l_2, 1), None, None]
        dz_all, loss_sum = None, 0.0
        dx_own, arrived, pending = [], [], []

        def forward(c):
            (in_a, in_b), (k_y, k_x, k_own) = arrived[c]
            add_a, add_b = k_y + in_a[HF:], k_x + in_b[HF:]
            pending.append((hop(add_a, 4), hop(add_b, 2)))
            return [add_a, add_b]

        for c in range(NCH):
            deps_out, deps_keep = [], []
            if c == 1:
                deps_out = [lse_3] + forward(0)
            if c == 2:
                deps_out = list(pending[0])
            if c == 3:
                deps_out = forward(1)
            (a_xy, b_xy), (a_dg, b_dg) = l_xy[c], l_dg[c]
            dz_all, pk1, send_a, send_b = local_grads(
                core_arr, w2, lab_c[c][:, :t], lse_c[c][:, :t], sc_c[c][:, :t], [(a_xy, CH, b_xy), (a_dg, CH, b_dg)], dz_all, 2 * c,
                send_outs, deps_out)
            incoming = (hop(send_a, 2), hop(send_b, 4))
            dz_all, pk2, k_y, k_x, k_own = local_grads(
                core_arr, w2, lab_c[c][:, t:], lse_c[c][:, t:], sc_c[c][:, t:], [(a_xy, CH, b_xy + 1), (l_own, CH, c)], dz_all, 2 * c + 1,
                keep_outs, deps_keep)
            arrived.append((incoming, (k_y, k_x, k_own)))
            pk = jnp.concatenate([pk1, pk2], axis=1)
            loss_sum = loss_sum + jnp.sum(jnp.where(lab_c[c] >= 0, lse_c[c] - pk, 0.0))
            if c == 0:
                l_3, lse_3, x_all = local_logits(
                    core_arr, w2, [x_d[2], x_d[3], x_x[3], x_y[3]],
                    [whole(2, DG, 0), whole(3, DG, 1), split(3, XN, 2), split(3, YN, 2)], x_all, [pk2])
                l_dg[2:] = [(l_3, 0), (l_3, 1)]
                l_xy[3] = (l_3, 2)
                lse_c += full_lse([
                    [blk(lse_2, 2), blk(lse_3, 0), blk(lse_2, 3), blk(lse_own, 2)],
                    [blk(lse_3, 2), blk(lse_3, 1), blk(lse_3, 3), blk(lse_own, 3)]])

        def dw_part(rows, cols):
            return jnp.einsum("vt,td->vd", dz_all[rows, cols], x_all[cols], preferred_element_type=F32)

        every, head, rest = slice(None), slice(0, 2 * NCH * CH), slice(2 * NCH * CH, None)
        forward(2)
        dz_all, *pending[1] = lax.optimization_barrier((dz_all, *pending[1]))
        dw_other = dw_part(slice(VD, None), every)
        arrived[3] = after(arrived[3], dw_other[:8, :128])
        forward(NCH - 1)
        dw_other = hop(dw_other, 1)
        x_all, *pending[2] = lax.optimization_barrier((x_all, *pending[2]))
        dw_mine = dw_part(slice(0, VD), head)
        pending[3] = after(pending[3], dw_mine[:8, :128])

        for c in range(NCH):
            (in_a, in_b), (_, _, k_own) = arrived[c]
            fin_a, fin_b = pending[c]
            dx_own.append(jnp.concatenate([k_own[:HF] + in_a[:HF] + fin_a, k_own[HF:] + in_b[:HF] + fin_b]))

        dg, dh = 0.0, []
        for c in range(NCH):
            gx = dx_own[c].astype(BF16).astype(F32)
            h = h_c[c].astype(F32)
            r = lax.rsqrt(jnp.mean(h * h, axis=-1, keepdims=True) + EPSILON)
            n = (h * r).astype(BF16).astype(F32)
            dg = dg + jnp.sum(gx * n, axis=0)
            gn = gx * gain
            proj = jnp.mean(gn * h, axis=-1, keepdims=True)
            dh.append((r * gn - h * r ** 3 * proj).astype(BF16))
        dz_all, dg = lax.optimization_barrier((dz_all, dg))
        grad_w = dw_part(slice(0, VD), rest) + (dw_mine + dw_other)
        tail = jnp.sum(lax.all_gather(jnp.concatenate([dg, jnp.full((128,), loss_sum, F32)]), AX), axis=0)
        grad_g = lax.dynamic_slice(tail, (me * (D // NDEV),), (D // NDEV,))
        loss_value = tail[D] / count
        return loss_value, jnp.concatenate(dh).reshape(nb, seq_len, D), grad_w, grad_g

    return jax.shard_map(local_step, mesh=mesh, in_specs=(P(AX, None, None), P(AX), P(AX, None), P(AX, None)), out_specs=(P(), P(AX, None, None), P(AX, None), P(AX)), check_vma=False)
```
